32 devices in a mesh: seq: 8 (over y, x, core), head: 4 (over z).
Axes of the slice: x: 2, y: 2, z: 4, core: 2. Of those that a mesh axis runs over, the one named last changes fastest.
Arguments:
- queries: bfloat16 [1024, 8192], P('seq', 'head'), may hold values from -2.5 to 2.5
- keys: bfloat16 [1024, 8192], P('seq', 'head'), may hold values from -2.5 to 2.5
- values: bfloat16 [1024, 4096], P('seq', 'head'), may hold values from -2.5 to 2.5
- out_grad: bfloat16 [1024, 4096], P('seq', 'head'), may hold values from -2.5 to 2.5
- log_gate: float32 [64, 1024], P('head', 'seq'), may hold values from -1 to 0
- level_weight: float32 [6, 64, 1024], P(None, 'head', 'seq'), may hold values from 0.25 to 2
- doc_start: int32 [1024], P('seq'), may hold values 0 or 1
Outputs:
- grad_queries: bfloat16 [1024, 8192], P('seq', 'head')
- grad_keys: bfloat16 [1024, 8192], P('seq', 'head')
- grad_values: bfloat16 [1024, 4096], P('seq', 'head')
- grad_level_weight: float32 [6, 64, 1024], P(None, 'head', 'seq')
- grad_log_gate: float32 [64, 1024], P('head', 'seq')
The draws below stay inside these ranges and needn't reach their ends.
All inputs are finite; a program needn't handle non-finite values. No bound on the sum of `doc_start` on one device may be relied on, other than what follows from the above.
Results may differ from the reference program's by a relative error of at most 0.0027.
Values sent between devices are 32-bit elements; how exact they have to be, the bound alone decides.
A program may use at most 128 MiB of HBM per device.

```python
import math
import jax
import jax.numpy as jnp
from jax import lax

HEAD_COUNT = 64
DK = 128
DV = 64
NL = 6
SPAN = 64
TOK_DEV = 128
TOKEN_COUNT = 1024
SPANS = 16


def draw_log_gate(key, part):
    every_key = jax.random.split(key, 7)
    slow_share = 0.5
    sluggish_head = jax.random.uniform(every_key[0], (HEAD_COUNT, 1)) < slow_share
    fast_rate = jnp.exp(jax.random.uniform(every_key[1], (HEAD_COUNT, 1), minval=jnp.log(0.02), maxval=jnp.log(0.05)))
    slow_rate = jnp.exp(jax.random.uniform(every_key[2], (HEAD_COUNT, 1), minval=jnp.log(0.1), maxval=jnp.log(0.56))) / TOKEN_COUNT
    block_count = TOKEN_COUNT // TOK_DEV
    block_factor = jnp.exp(jax.random.uniform(every_key[3], (HEAD_COUNT, block_count), minval=jnp.log(0.5), maxval=jnp.log(2.0)))
    block_factor = jnp.repeat(block_factor, TOK_DEV, axis=1)
    rough = jax.random.uniform(every_key[4], (HEAD_COUNT, TOKEN_COUNT), minval=0.5, maxval=2.0)
    decay_speed = jnp.where(sluggish_head, slow_rate, fast_rate * block_factor) * rough
    spike_position = jax.random.randint(every_key[5], (3,), 0, TOKEN_COUNT)
    spike_struck = jnp.any(jnp.arange(TOKEN_COUNT)[None, :] == spike_position[:, None], axis=0)
    spike_length = jnp.log(1.0 - jax.random.uniform(every_key[6], (HEAD_COUNT, 1), minval=0.2, maxval=0.4))
    spike_event = jnp.where(sluggish_head & spike_struck[None, :], spike_length, 0.0)
    return (spike_event - decay_speed).astype(jnp.float32)


def place_ends(values, rng, smallest, top_value):
    spot = [jax.random.randint(jax.random.fold_in(rng, axis), (), 0, length) for axis, length in enumerate(values.shape)]
    longest = values.shape.index(max(values.shape))
    neighbour = spot[:longest] + [(spot[longest] + 1) % values.shape[longest]] + spot[longest + 1:]
    return values.at[tuple(spot)].set(smallest).at[tuple(neighbour)].set(top_value)


def block_scale(key, dims, cuts, smallest, largest):
    loudness, own = 1.0, jax.random.fold_in(key, 6)
    for dim, shards_of in cuts:
        draws = jnp.exp(jax.random.uniform(jax.random.fold_in(own, dim), (shards_of,), jnp.float32, smallest / len(cuts), largest / len(cuts)))
        loudness = loudness * jnp.repeat(draws, dims[dim] // shards_of).reshape([-1 if axis == dim else 1 for axis in range(len(dims))])
    return loudness


def scatter_about(rng, extent, deviation, reach, shards=(), dtype=jnp.bfloat16):
    result = jax.random.normal(rng, extent, jnp.float32) * deviation
    if len(shards) > 0:
        result = block_scale(rng, extent, shards, -0.22, 0.18) * result
    return jnp.clip(result, min=-reach, max=reach).astype(dtype)


def setup_inputs(seed: int = 0) -> dict:
    key_of = jax.random.split(jax.random.key(seed), 8)
    return {
        "queries": scatter_about(key_of[0], (TOKEN_COUNT, HEAD_COUNT * DK), 0.16, 2.5, ((0, 8), (1, 4))),
        "keys": scatter_about(key_of[1], (TOKEN_COUNT, HEAD_COUNT * DK), 0.16, 2.5, ((0, 8), (1, 4))),
        "values": scatter_about(key_of[2], (TOKEN_COUNT, HEAD_COUNT * DV), 0.16, 2.5, ((0, 8), (1, 4))),
        "out_grad": scatter_about(key_of[3], (TOKEN_COUNT, HEAD_COUNT * DV), 0.16, 2.5, ((0, 8), (1, 4))),
        "log_gate": draw_log_gate(jax.random.fold_in(key_of[7], 71), 0),
        "level_weight": jnp.clip(jnp.exp(math.log(2.0) - 2.0794415 * jax.random.uniform(key_of[5], (NL, HEAD_COUNT, TOKEN_COUNT), jnp.float32) ** block_scale(key_of[5], (NL, HEAD_COUNT, TOKEN_COUNT), ((1, 4), (2, 8)), -0.2, 0.2)), 0.25, 2.0),
        "doc_start": place_ends((jax.random.randint(key_of[6], (TOKEN_COUNT,), 0, TOK_DEV * 8) < 1).astype(jnp.int32), jax.random.fold_in(key_of[6], 1), 0, 1),
    }


exact_mode = lax.Precision.HIGHEST

def group_sums(span_log, span_dead, width):
    groups = span_log.shape[0] // width
    logs = span_log.reshape(groups, width)
    deads = span_dead.reshape(groups, width)
    return (jnp.cumsum(logs, axis=1), jnp.cumsum(deads, axis=1), logs, deads)

def fenwick_pull(states, span_log, span_dead):
    total = states.shape[1]
    rows = states.shape[2]
    cols = states.shape[3]
    pieces = [jnp.zeros((total, rows, cols), jnp.float32)]
    for level in range(1, NL - 1):
        width = 2 ** (level - 1)
        groups = total // (2 * width)
        cum_log, cum_dead, logs, deads = group_sums(span_log, span_dead, 2 * width)
        source = states[level].reshape(groups, 2 * width, rows, cols)[:, :width]
        reach_log = cum_log[:, width - 1:2 * width - 1]
        reach_dead = cum_dead[:, width - 1:2 * width - 1]
        same = reach_dead[:, :, None] == cum_dead[:, None, :width]
        gap = reach_log[:, :, None] - cum_log[:, None, :width]
        weight = jnp.where(same, jnp.exp(jnp.where(same, gap, 0.0)), 0.0)
        pulled = jnp.einsum('gis,gsde->gide', weight, source, precision=exact_mode)
        pieces.append(jnp.concatenate([jnp.zeros_like(pulled), pulled], axis=1).reshape(total, rows, cols))
    width = 2 ** (NL - 2)
    groups = total // width
    cum_log, cum_dead, logs, deads = group_sums(span_log, span_dead, width)
    source = states[NL - 1].reshape(groups, width, rows, cols)
    end_same = cum_dead[:, -1:] == cum_dead
    end_weight = jnp.where(end_same, jnp.exp(jnp.where(end_same, cum_log[:, -1:] - cum_log, 0.0)), 0.0)
    block_total = jnp.einsum('gs,gsde->gde', end_weight, source, precision=exact_mode)
    block_decay = jnp.exp(cum_log[:, -1]) * (cum_dead[:, -1] == 0).astype(jnp.float32)

    def carry_step(carry, inputs):
        decay_now, total_now = inputs
        return (decay_now * carry + total_now, carry)
    _, entering = lax.scan(carry_step, jnp.zeros((rows, cols), jnp.float32), (block_decay, block_total))
    lead = jnp.exp(cum_log - logs) * (cum_dead - deads == 0).astype(jnp.float32)
    pieces.append((lead[:, :, None, None] * entering[:, None]).reshape(total, rows, cols))
    return jnp.stack(pieces)

def head_pass(query_h, key_h, value_h, grad_h, gate_h, weight_h, start_all):
    positions = jnp.arange(SPAN)
    causal = positions[:, None] >= positions[None, :]
    cum_gate = jnp.cumsum(gate_h, axis=1)
    cum_reset = jnp.cumsum(start_all, axis=1)
    valid = causal[None] & (cum_reset[:, :, None] == cum_reset[:, None, :])
    gap = cum_gate[:, :, None] - cum_gate[:, None, :]
    decay_in = jnp.where(valid, jnp.exp(jnp.where(valid, gap, 0.0)), 0.0)
    from_start = jnp.exp(cum_gate) * (cum_reset == 0).astype(jnp.float32)
    to_end = jnp.exp(cum_gate[:, -1:] - cum_gate) * (cum_reset == cum_reset[:, -1:]).astype(jnp.float32)
    span_log = cum_gate[:, -1]
    span_dead = (cum_reset[:, -1] > 0).astype(jnp.int32)
    query_f = query_h.astype(jnp.float32)
    key_f = key_h.astype(jnp.float32)
    value_f = value_h.astype(jnp.float32)
    grad_f = grad_h.astype(jnp.float32)
    scores = jnp.einsum('ctd,csd->cts', query_f, key_f, precision=exact_mode)
    grad_dot = jnp.einsum('cte,cse->cts', grad_f, value_f, precision=exact_mode)
    weighted = decay_in * weight_h[0][:, :, None]
    prob_mix = (weighted * scores).astype(jnp.bfloat16)
    grad_mix = (weighted * grad_dot).astype(jnp.bfloat16)
    intra = lax.optimization_barrier(jnp.sum(decay_in * scores * grad_dot, axis=2))
    end_col = to_end[:, :, None]
    span_state = jnp.einsum('csd,cse->cde', key_f * end_col, value_f, precision=exact_mode)
    forward = fenwick_pull(jnp.broadcast_to(span_state[None], (NL,) + span_state.shape), span_log, span_dead)
    query_state = jnp.einsum('ctd,lcde->lcte', query_f, forward, precision=exact_mode)
    lam_start = weight_h * from_start[None]
    out_in = jnp.einsum('lcte,lct->cte', query_state, lam_start, precision=exact_mode)
    level_in = jnp.einsum('lcte,cte->lct', query_state, grad_f, precision=exact_mode) * from_start[None]
    grad_weighted = lam_start[:, :, :, None] * grad_f[None]
    query_in = jnp.einsum('lcte,lcde->ctd', grad_weighted, forward, precision=exact_mode)
    out_loc = jnp.einsum('cts,cse->cte', prob_mix.astype(jnp.float32), value_f, precision=exact_mode)
    query_loc = jnp.einsum('cts,csd->ctd', grad_mix.astype(jnp.float32), key_f, precision=exact_mode)
    outputs = out_loc + out_in
    grad_query = (query_loc + query_in).astype(jnp.bfloat16)
    level_zero = (jnp.arange(NL) == 0).astype(jnp.float32)
    grad_level = level_in + level_zero[:, None, None] * intra[None]
    lam_query = lam_start[:, :, :, None] * query_f[None]
    back_local = jnp.einsum('lctd,cte->lcde', lam_query, grad_f, precision=exact_mode)
    backward = fenwick_pull(back_local[:, ::-1], span_log[::-1], span_dead[::-1])[:, ::-1]
    back_sum = lax.optimization_barrier(jnp.sum(backward, axis=0))
    key_in = jnp.einsum('cse,cde->csd', value_f * end_col, back_sum, precision=exact_mode)
    value_in = jnp.einsum('csd,cde->cse', key_f * end_col, back_sum, precision=exact_mode)
    key_loc = jnp.einsum('cts,ctd->csd', grad_mix.astype(jnp.float32), query_f, precision=exact_mode)
    value_loc = jnp.einsum('cts,cte->cse', prob_mix.astype(jnp.float32), grad_f, precision=exact_mode)
    value_grad = value_loc + value_in
    drift = lax.optimization_barrier(jnp.sum(grad_f * outputs, axis=2)) - lax.optimization_barrier(jnp.sum(value_f * value_grad, axis=2))
    return (grad_query, (key_loc + key_in).astype(jnp.bfloat16), value_grad.astype(jnp.bfloat16), grad_level, drift)

def reference(queries, keys, values, out_grad, log_gate, level_weight, doc_start):
    query_all = queries.reshape(SPANS, SPAN, HEAD_COUNT, DK).transpose(2, 0, 1, 3)
    key_all = keys.reshape(SPANS, SPAN, HEAD_COUNT, DK).transpose(2, 0, 1, 3)
    value_all = values.reshape(SPANS, SPAN, HEAD_COUNT, DV).transpose(2, 0, 1, 3)
    grad_all = out_grad.reshape(SPANS, SPAN, HEAD_COUNT, DV).transpose(2, 0, 1, 3)
    gate_all = log_gate.reshape(HEAD_COUNT, SPANS, SPAN)
    start_all = doc_start.reshape(SPANS, SPAN)
    weight_all = level_weight.reshape(NL, HEAD_COUNT, SPANS, SPAN).transpose(1, 0, 2, 3)

    def one_head(inputs):
        query_h, key_h, value_h, grad_h, gate_h, weight_h = inputs
        return head_pass(query_h, key_h, value_h, grad_h, gate_h, weight_h, start_all)
    results = lax.map(one_head, (query_all, key_all, value_all, grad_all, gate_all, weight_all))
    grad_query, grad_key, grad_value, grad_level, drift = results
    grad_queries = grad_query.transpose(1, 2, 0, 3).reshape(TOKEN_COUNT, HEAD_COUNT * DK)
    grad_keys = grad_key.transpose(1, 2, 0, 3).reshape(TOKEN_COUNT, HEAD_COUNT * DK)
    grad_values = grad_value.transpose(1, 2, 0, 3).reshape(TOKEN_COUNT, HEAD_COUNT * DV)
    grad_level_weight = grad_level.transpose(1, 0, 2, 3).reshape(NL, HEAD_COUNT, TOKEN_COUNT)
    drift_term = drift.reshape(HEAD_COUNT, TOKEN_COUNT)
    tail = lax.cumsum(drift_term, axis=1, reverse=True)
    squares = jnp.sum(tail * tail)
    factor = jnp.minimum(1.0, lax.rsqrt(squares / (HEAD_COUNT * TOKEN_COUNT) + 1e-06))
    return (grad_queries, grad_keys, grad_values, grad_level_weight, tail * factor)
```

```python
import functools

import jax
import jax.numpy as jnp
from jax import lax
from jax.experimental import pallas as pl
from jax.experimental.pallas import tpu as pltpu
from jax.sharding import PartitionSpec as P

SPAN = 64
F32 = jnp.float32
BF16 = jnp.bfloat16
NN = (((1,), (0,)), ((), ()))
NT = (((1,), (1,)), ((), ()))
TN = (((0,), (0,)), ((), ()))
MESH = pl.DeviceIdType.MESH


def dot(a, b, dims):
    return lax.dot_general(a, b, dims, preferred_element_type=F32)


def split(x):
    high = x.astype(BF16)
    return high, (x - high.astype(F32)).astype(BF16)


def dot_fine(x, b, dims):
    high, low = split(x)
    return dot(high, b, dims) + dot(low, b, dims)


def span_level(a, b, levels):
    return 0 if a == b else min(levels - 1, (a ^ b).bit_length())


def kernel(
    seq_count,
    head_count,
    q_ref,
    k_ref,
    v_ref,
    g_ref,
    lg_ref,
    lw_ref,
    ds_ref,
    gq_ref,
    gk_ref,
    gv_ref,
    gl_ref,
    gg_ref,
    cum_s,
    col_s,
    lead_s,
    tail_s,
    bias_s,
    vt_s,
    gt_s,
    vg_s,
    gq_s,
    gk_s,
    drift_s,
    coef_s,
    state_s,
    back_s,
    lvl,
    got_s,
    got_u,
    sum_s,
    sum_u,
    dec,
    got_dec,
    tot,
    sq,
    lvl_send,
    lvl_recv,
    fwd_send,
    fwd_recv,
    s_send,
    s_recv,
    u_send,
    u_recv,
    d_send,
    d_recv,
    t_send,
    t_recv,
    q_send,
    q_recv,
):
    tok = q_ref.shape[0]
    heads = lg_ref.shape[0]
    levels = lw_ref.shape[0]
    dk = q_ref.shape[1] // heads
    dv = v_ref.shape[1] // heads
    group = dk // dv
    pairs = heads // group
    spans = tok // SPAN
    span_bits = spans.bit_length() - 1
    bits = seq_count.bit_length() - 1
    half = heads // 2
    cross = [min(span_bits + 1 + b, levels - 1) for b in range(bits)]
    slots = sorted(set(cross))
    place = lax.axis_index("seq")
    row = lax.axis_index("head")
    bit = [(place // (1 << b)) % 2 for b in range(bits)]
    peer = [place + (1 - 2 * bit[b]) * (1 << b) for b in range(bits)]
    want_s = [(place // (2 << b)) != (seq_count // (2 << b)) - 1 for b in range(bits)]
    mine = bit[0] * half
    theirs = (1 - bit[0]) * half

    barrier = pltpu.get_barrier_semaphore()
    for o in range(1, seq_count):
        pl.semaphore_signal(
            barrier, inc=1, device_id={"seq": (place + o) % seq_count}, device_id_type=MESH
        )
    for o in range(1, head_count):
        pl.semaphore_signal(
            barrier, inc=1, device_id={"head": (row + o) % head_count}, device_id_type=MESH
        )

    rows_i = lax.broadcasted_iota(jnp.int32, (tok, tok), 0)
    cols_i = lax.broadcasted_iota(jnp.int32, (tok, tok), 1)
    tri = (rows_i <= cols_i).astype(F32)
    starts = jnp.broadcast_to(ds_ref[...].astype(F32), (8, tok))
    both = jnp.concatenate([lg_ref[...], starts], axis=0)
    cum_all = lax.dot_general(
        both, tri, NN, precision=lax.Precision.HIGHEST, preferred_element_type=F32
    )
    cum_t = jnp.transpose(cum_all)
    cum = cum_all[:heads]
    reset = cum_all[heads : heads + 1]
    reset_col = cum_t[:, heads : heads + 1]
    bias_s[...] = jnp.where((rows_i <= cols_i) & (reset == reset_col), 0.0, -1e30)
    end = cum[:, tok - 1 : tok]
    reset_end = reset[:, tok - 1 : tok]
    cum_s[...] = cum
    lead_s[...] = jnp.where(reset == 0, jnp.exp(cum), 0.0)
    tail_s[...] = jnp.where(reset == reset_end, jnp.exp(end - cum), 0.0)
    dec[0] = jnp.broadcast_to(jnp.where(reset_end == 0, jnp.exp(end), 0.0), (heads, dk))
    for h in range(heads):
        col_s[h] = jnp.broadcast_to(cum_t[:, h : h + 1], (tok, tok))

    def states(p, _):
        lanes = pl.ds(pl.multiple_of(p * dk, dk), dk)
        vt = jnp.transpose(v_ref[:, lanes].astype(F32))
        gt = jnp.transpose(g_ref[:, lanes].astype(F32))
        vt_s[p] = vt.astype(BF16)
        gt_s[p] = gt.astype(BF16)
        for i in range(group):
            h = p * group + i
            wide = pl.ds(pl.multiple_of(h * dk, dk), dk)
            part = slice(i * dv, (i + 1) * dv)
            tail = tail_s[pl.ds(h, 1), :]
            lead = lead_s[pl.ds(h, 1), :]
            state_s[h] = dot_fine(vt[part] * tail, k_ref[:, wide], NN)
            gw = jnp.concatenate(
                [gt[part] * (lead * lw_ref[l, pl.ds(h, 1), :]) for l in slots], axis=0
            )
            back = dot_fine(gw, q_ref[:, wide], NN)
            for n in range(len(slots)):
                back_s[n, h] = back[n * dv : (n + 1) * dv]
        return 0

    lax.fori_loop(0, pairs, states, 0)
    pl.semaphore_wait(barrier, seq_count - 1 + head_count - 1)

    def slot(b):
        return slots.index(cross[b])

    def remote(src, dst, send, recv, b):
        return pltpu.make_async_remote_copy(
            src_ref=src,
            dst_ref=dst,
            send_sem=send,
            recv_sem=recv,
            device_id={"seq": peer[b]},
            device_id_type=MESH,
        )

    own = pl.ds(mine, half)
    other = pl.ds(theirs, half)

    def u_copy(b, j):
        src = back_s.at[slot(j), other] if b == 0 else sum_u.at[b, j]
        return remote(src, got_u.at[b, j], u_send.at[b, j], u_recv.at[b, j], b)

    def s_copy(b):
        src = state_s.at[other] if b == 0 else sum_s.at[b]
        return remote(src, got_s.at[b], s_send.at[b], s_recv.at[b], b)

    def d_copy(b):
        return remote(dec.at[b], got_dec.at[b], d_send.at[b], d_recv.at[b], b)

    def level_copy(b, low):
        if b == 0:
            src = state_s if low else back_s.at[slot(0)]
            return [
                remote(src.at[part], lvl.at[0, part], lvl_send.at[0, n], lvl_recv.at[0, n], 0)
                for n, part in enumerate((other, own))
            ]
        src = sum_s.at[b] if low else sum_u.at[b, b]
        return [remote(src, lvl.at[b, own], lvl_send.at[b, 0], lvl_recv.at[b, 0], b)]

    def level_wait(b, n):
        part = other if n == 1 else own
        return remote(
            lvl.at[b, part], lvl.at[b, part], lvl_send.at[b, n], lvl_recv.at[b, n], b
        )

    def forward_copy(b, part):
        return remote(lvl.at[b, part], lvl.at[b, part], fwd_send.at[b], fwd_recv.at[b], 0)

    def begin(b):
        d_copy(b).start()

        @pl.when(bit[b] == 0)
        def _():
            for c in level_copy(b, True):
                c.start()

        if b < bits - 1:

            @pl.when((bit[b] == 1) & want_s[b])
            def _():
                s_copy(b).start()

            for j in range(b + 1, bits):

                @pl.when(bit[j] == 1)
                def _(j=j):
                    u_copy(b, j).start()

        @pl.when(bit[b] == 1)
        def _():
            for c in level_copy(b, False):
                c.start()

    def join(b):
        d_copy(b).wait_recv()
        level_wait(b, 0).wait_recv()
        if b > 0:
            forward_copy(b, own).start()
        up = bit[b].astype(F32)
        got = got_dec[b]
        now = dec[b]
        dec[b + 1] = got * now
        if b == bits - 1:
            return
        base_s = state_s.at[own] if b == 0 else sum_s.at[b]

        @pl.when(want_s[b])
        def _():
            @pl.when(bit[b] == 1)
            def _():
                def body(i, _):
                    d = dec[b, pl.ds(mine + i, 1), :]
                    sum_s[b + 1, i] = d * lvl[b, mine + i] + base_s[i]
                    return 0

                lax.fori_loop(0, half, body, 0, unroll=True)

            @pl.when(bit[b] == 0)
            def _():
                s_copy(b).wait_recv()

                def body(i, _):
                    d = got_dec[b, pl.ds(mine + i, 1), :]
                    sum_s[b + 1, i] = d * base_s[i] + got_s[b, i]
                    return 0

                lax.fori_loop(0, half, body, 0, unroll=True)

        for j in range(b + 1, bits):
            base_u = back_s.at[slot(j), own] if b == 0 else sum_u.at[b, j]

            @pl.when(bit[j] == 1)
            def _(j=j, base_u=base_u):
                u_copy(b, j).wait_recv()

                def body(i, _):
                    d0 = dec[b, pl.ds(mine + i, 1), :]
                    d1 = got_dec[b, pl.ds(mine + i, 1), :]
                    a = up * d1 + (1.0 - up)
                    c = (1.0 - up) * d0 + up
                    sum_u[b + 1, j, i] = a * base_u[i] + c * got_u[b, j, i]
                    return 0

                lax.fori_loop(0, half, body, 0, unroll=True)

    span_of = lax.broadcasted_iota(jnp.int32, (1, tok), 1) // SPAN

    def local(p, _):
        vt = vt_s[p]
        gt = gt_s[p]
        lanes = pl.ds(pl.multiple_of(p * dk, dk), dk)
        v_blk = v_ref[:, lanes]
        for i in range(group):
            h = p * group + i
            wide = pl.ds(pl.multiple_of(h * dk, dk), dk)
            part = slice(i * dv, (i + 1) * dv)
            q = q_ref[:, wide]
            k = k_ref[:, wide]
            score = dot(k, q, NT)
            pair = dot(v_blk[:, part], gt[part], NN)
            decay = jnp.exp((cum_s[pl.ds(h, 1), :] - col_s[h]) + bias_s[...])
            seen = decay * score
            both_p = seen * pair
            gains = [lw_ref[l, pl.ds(h, 1), :] for l in range(span_bits + 1)]
            level_rows = [jnp.zeros((1, tok), F32) for _ in range(span_bits + 1)]
            mixed, graded = [], []
            for cs in range(spans):
                rows = slice(cs * SPAN, (cs + 1) * SPAN)
                total = jnp.sum(both_p[rows], axis=0, keepdims=True)
                gain = jnp.zeros((1, tok), F32)
                for ct in range(cs, spans):
                    l = span_level(cs, ct, levels)
                    hit = span_of == ct
                    gain = jnp.where(hit, gains[l], gain)
                    level_rows[l] = level_rows[l] + jnp.where(hit, total, 0.0)
                mixed.append(seen[rows] * gain)
                graded.append(decay[rows] * gain * pair[rows])
            mix = jnp.concatenate(mixed, axis=0).astype(BF16)
            grade = jnp.concatenate(graded, axis=0).astype(BF16)
            for l in range(span_bits + 1):
                gl_ref[l, pl.ds(h, 1), :] = level_rows[l]
            drift_s[pl.ds(h, 1), :] = jnp.sum(mix.astype(F32) * pair, axis=0, keepdims=True)
            vg_s[p, part] = dot(gt[part], mix, NT)
            gk_s[h] = dot(grade, q, NN)
            gq_s[h] = dot(grade, k, TN)
        return 0

    begin(0)
    lax.fori_loop(0, pairs // 2, local, 0)
    join(0)
    if bits > 1:
        begin(1)
    lax.fori_loop(pairs // 2, pairs, local, 0)
    for b in range(1, bits):
        join(b)
        if b + 1 < bits:
            begin(b + 1)

    inner_f = jnp.ones((heads, dk), F32)
    inner_b = jnp.ones((heads, dk), F32)
    for b in range(bits):
        up = bit[b].astype(F32)
        got = got_dec[b]
        coef_s[0, b] = inner_f * up
        coef_s[1, b] = inner_b * (1.0 - up)
        inner_f = inner_f * (up * got + (1.0 - up))
        inner_b = inner_b * ((1.0 - up) * got + up)
    level_wait(0, 1).wait_recv()
    for b in range(1, bits):
        forward_copy(b, other).wait_recv()

    def finish(p, _):
        lanes = pl.ds(pl.multiple_of(p * dk, dk), dk)
        vt = vt_s[p].astype(F32)
        gt = gt_s[p].astype(F32)
        vg_all = []
        for i in range(group):
            h = p * group + i
            wide = pl.ds(pl.multiple_of(h * dk, dk), dk)
            part = slice(i * dv, (i + 1) * dv)
            q = q_ref[:, wide]
            k = k_ref[:, wide]
            tail = tail_s[pl.ds(h, 1), :]
            lead = lead_s[pl.ds(h, 1), :]
            blocks = [lvl[b, h] for b in range(bits)]
            entering = []
            for n in range(len(slots)):
                terms = [
                    coef_s[0, b, pl.ds(h, 1), :] * blocks[b] for b in range(bits) if slot(b) == n
                ]
                entering.append(functools.reduce(jnp.add, terms))
            entering = jnp.concatenate(entering, axis=0)
            after = functools.reduce(
                jnp.add, [coef_s[1, b, pl.ds(h, 1), :] * blocks[b] for b in range(bits)]
            )
            e_high, e_low = split(entering)
            seen = dot(e_high, q, NT) + dot(e_low, q, NT)
            drift = drift_s[pl.ds(h, 1), :]
            gws = []
            for n, l in enumerate(slots):
                gain = lw_ref[l, pl.ds(h, 1), :]
                level = lead * jnp.sum(
                    seen[n * dv : (n + 1) * dv] * gt[part], axis=0, keepdims=True
                )
                gl_ref[l, pl.ds(h, 1), :] = level
                drift = drift + gain * level
                gws.append(gt[part] * (lead * gain))
            gw, gw_low = split(jnp.concatenate(gws, axis=0))
            gq_in = dot(gw, e_high, TN) + dot(gw, e_low, TN) + dot(gw_low, e_high, TN)
            gq_ref[:, wide] = (gq_s[h] + gq_in).astype(BF16)
            a_high, a_low = split(after)
            tv, tv_low = split(vt[part] * tail)
            gk_in = dot(tv, a_high, TN) + dot(tv, a_low, TN) + dot(tv_low, a_high, TN)
            gk_ref[:, wide] = (gk_s[h] + gk_in).astype(BF16)
            vg = vg_s[p, part] + tail * (dot(a_high, k, NT) + dot(a_low, k, NT))
            drift_s[pl.ds(h, 1), :] = drift - jnp.sum(vg * vt[part], axis=0, keepdims=True)
            vg_all.append(vg)
        gv_ref[:, lanes] = jnp.transpose(jnp.concatenate(vg_all, axis=0)).astype(BF16)
        return 0

    lax.fori_loop(0, pairs, finish, 0)
    for l in range(levels):
        if l > span_bits and l not in slots:
            gl_ref[l] = jnp.zeros((heads, tok), F32)

    later = (rows_i >= cols_i).astype(F32)
    local_tail = lax.dot_general(
        drift_s[...], later, NN, precision=lax.Precision.HIGHEST, preferred_element_type=F32
    )
    lane = lax.broadcasted_iota(jnp.int32, (heads, tok), 1)
    first = local_tail[:, 0:1]
    plain = jnp.sum(local_tail, axis=1, keepdims=True)
    square = jnp.sum(local_tail * local_tail, axis=1, keepdims=True)
    tot[place] = jnp.where(lane == 0, first, jnp.where(lane == 1, plain, square))

    def tot_copy(o, slot_at):
        return pltpu.make_async_remote_copy(
            src_ref=tot.at[place],
            dst_ref=tot.at[slot_at],
            send_sem=t_send.at[o],
            recv_sem=t_recv.at[slot_at],
            device_id={"seq": (place + o) % seq_count},
            device_id_type=MESH,
        )

    for o in range(1, seq_count):
        tot_copy(o, place).start()
    for o in range(1, seq_count):
        tot_copy(o, (place + o) % seq_count).wait_recv()
    after_total = jnp.zeros((heads, 1), F32)
    my_later = jnp.zeros((heads, 1), F32)
    energy = jnp.zeros((heads, 1), F32)
    for d in reversed(range(seq_count)):
        piece = tot[d]
        my_later = my_later + jnp.where(place == d, 1.0, 0.0) * after_total
        energy = energy + (
            piece[:, 2:3] + after_total * (2.0 * piece[:, 1:2] + tok * after_total)
        )
        after_total = after_total + piece[:, 0:1]
    energy = jnp.sum(jnp.broadcast_to(energy, (heads, dk)), axis=0, keepdims=True)
    sq[row] = jnp.broadcast_to(energy, (8, dk))

    def sq_copy(o, slot_at):
        return pltpu.make_async_remote_copy(
            src_ref=sq.at[row],
            dst_ref=sq.at[slot_at],
            send_sem=q_send.at[o],
            recv_sem=q_recv.at[slot_at],
            device_id={"head": (row + o) % head_count},
            device_id_type=MESH,
        )

    for o in range(1, head_count):
        sq_copy(o, row).start()
    for o in range(1, head_count):
        sq_copy(o, (row + o) % head_count).wait_recv()
    whole = sq[0]
    for r in range(1, head_count):
        whole = whole + sq[r]
    count = heads * tok * seq_count * head_count
    factor = jnp.minimum(1.0, lax.rsqrt(whole[0:1] / count + 1e-6))
    gg_ref[...] = (local_tail + my_later) * factor

    for b in range(bits):
        d_copy(b).wait_send()
        for n in range(2 if b == 0 else 1):
            level_wait(b, n).wait_send()
        if b > 0:
            forward_copy(b, own).wait_send()
        if b < bits - 1:

            @pl.when((bit[b] == 1) & want_s[b])
            def _(b=b):
                s_copy(b).wait_send()

            for j in range(b + 1, bits):

                @pl.when(bit[j] == 1)
                def _(b=b, j=j):
                    u_copy(b, j).wait_send()

    for o in range(1, seq_count):
        tot_copy(o, place).wait_send()
    for o in range(1, head_count):
        sq_copy(o, row).wait_send()


def shards(seq_count, head_count, queries, keys, values, out_grad, log_gate, level_weight, doc_start):
    tok = queries.shape[0]
    heads = log_gate.shape[0]
    levels = level_weight.shape[0]
    dk = queries.shape[1] // heads
    dv = values.shape[1] // heads
    group = dk // dv
    pairs = heads // group
    bits = seq_count.bit_length() - 1
    half = heads // 2
    span_bits = (tok // SPAN).bit_length() - 1
    slots = len({min(span_bits + 1 + b, levels - 1) for b in range(bits)})
    dma = pltpu.SemaphoreType.DMA
    vmem = pltpu.VMEM
    block = (dv, dk)
    scratch = [
        vmem((heads, tok), F32),
        vmem((heads, tok, tok), F32),
        vmem((heads, tok), F32),
        vmem((heads, tok), F32),
        vmem((tok, tok), F32),
        vmem((pairs, group * dv, tok), BF16),
        vmem((pairs, group * dv, tok), BF16),
        vmem((pairs, group * dv, tok), F32),
        vmem((heads, tok, dk), F32),
        vmem((heads, tok, dk), F32),
        vmem((heads, tok), F32),
        vmem((2, bits, heads, dk), F32),
        vmem((heads,) + block, F32),
        vmem((slots, heads) + block, F32),
        vmem((bits, heads) + block, F32),
        vmem((bits, half) + block, F32),
        vmem((bits, bits, half) + block, F32),
        vmem((bits, half) + block, F32),
        vmem((bits, bits, half) + block, F32),
        vmem((bits + 1, heads, dk), F32),
        vmem((bits, heads, dk), F32),
        vmem((seq_count, heads, tok), F32),
        vmem((head_count, 8, dk), F32),
        dma((bits, 2)),
        dma((bits, 2)),
        dma((bits,)),
        dma((bits,)),
        dma((bits,)),
        dma((bits,)),
        dma((bits, bits)),
        dma((bits, bits)),
        dma((bits,)),
        dma((bits,)),
        dma((seq_count,)),
        dma((seq_count,)),
        dma((head_count,)),
        dma((head_count,)),
    ]
    spec = pl.BlockSpec(memory_space=pltpu.VMEM)
    return pl.pallas_call(
        functools.partial(kernel, seq_count, head_count),
        out_shape=(
            jax.ShapeDtypeStruct(queries.shape, BF16),
            jax.ShapeDtypeStruct(keys.shape, BF16),
            jax.ShapeDtypeStruct(values.shape, BF16),
            jax.ShapeDtypeStruct(level_weight.shape, F32),
            jax.ShapeDtypeStruct(log_gate.shape, F32),
        ),
        in_specs=[spec] * 7,
        out_specs=(spec,) * 5,
        scratch_shapes=scratch,
        compiler_params=pltpu.CompilerParams(collective_id=0, has_side_effects=True),
    )(queries, keys, values, out_grad, log_gate, level_weight, doc_start.reshape(1, tok))


def solution(mesh):
    return jax.shard_map(
        functools.partial(shards, mesh.shape["seq"], mesh.shape["head"]),
        mesh=mesh,
        in_specs=(
            P("seq", "head"),
            P("seq", "head"),
            P("seq", "head"),
            P("seq", "head"),
            P("head", "seq"),
            P(None, "head", "seq"),
            P("seq"),
        ),
        out_specs=(
            P("seq", "head"),
            P("seq", "head"),
            P("seq", "head"),
            P(None, "head", "seq"),
            P("head", "seq"),
        ),
        check_vma=False,
    )
```

```python
import functools

import jax
import jax.numpy as jnp
from jax import lax
from jax.experimental import pallas as pl
from jax.experimental.pallas import tpu as pltpu
from jax.sharding import PartitionSpec as P

SPAN = 64
F32 = jnp.float32
BF16 = jnp.bfloat16
NN = (((1,), (0,)), ((), ()))
NT = (((1,), (1,)), ((), ()))
TN = (((0,), (0,)), ((), ()))
MESH = pl.DeviceIdType.MESH


def dot(a, b, dims):
    return lax.dot_general(a, b, dims, preferred_element_type=F32)


def split(x):
    high = x.astype(BF16)
    return high, (x - high.astype(F32)).astype(BF16)


def dot_fine(x, b, dims):
    high, low = split(x)
    return dot(high, b, dims) + dot(low, b, dims)


def span_level(a, b, levels):
    return 0 if a == b else min(levels - 1, (a ^ b).bit_length())


def kernel(
    seq_count,
    head_count,
    q_ref,
    k_ref,
    v_ref,
    g_ref,
    lg_ref,
    lw_ref,
    ds_ref,
    gq_ref,
    gk_ref,
    gv_ref,
    gl_ref,
    gg_ref,
    cum_s,
    col_s,
    lead_s,
    tail_s,
    bias_s,
    vt_s,
    gt_s,
    vg_s,
    gq_s,
    gk_s,
    drift_s,
    coef_s,
    state_s,
    back_s,
    lvl,
    got_s,
    got_u,
    sum_s,
    sum_u,
    dec,
    got_dec,
    tot,
    sq,
    lvl_send,
    lvl_recv,
    fwd_send,
    fwd_recv,
    s_send,
    s_recv,
    u_send,
    u_recv,
    d_send,
    d_recv,
    t_send,
    t_recv,
    q_send,
    q_recv,
):
    tok = q_ref.shape[0]
    heads = lg_ref.shape[0]
    levels = lw_ref.shape[0]
    dk = q_ref.shape[1] // heads
    dv = v_ref.shape[1] // heads
    group = dk // dv
    pairs = heads // group
    spans = tok // SPAN
    span_bits = spans.bit_length() - 1
    bits = seq_count.bit_length() - 1
    half = heads // 2
    cross = [min(span_bits + 1 + b, levels - 1) for b in range(bits)]
    slots = sorted(set(cross))
    place = lax.axis_index("seq")
    row = lax.axis_index("head")
    bit = [(place // (1 << b)) % 2 for b in range(bits)]
    peer = [place + (1 - 2 * bit[b]) * (1 << b) for b in range(bits)]
    want_s = [(place // (2 << b)) != (seq_count // (2 << b)) - 1 for b in range(bits)]
    mine = bit[0] * half
    theirs = (1 - bit[0]) * half

    barrier = pltpu.get_barrier_semaphore()
    for o in range(1, seq_count):
        pl.semaphore_signal(
            barrier, inc=1, device_id={"seq": (place + o) % seq_count}, device_id_type=MESH
        )
    for o in range(1, head_count):
        pl.semaphore_signal(
            barrier, inc=1, device_id={"head": (row + o) % head_count}, device_id_type=MESH
        )

    rows_i = lax.broadcasted_iota(jnp.int32, (tok, tok), 0)
    cols_i = lax.broadcasted_iota(jnp.int32, (tok, tok), 1)
    tri = (rows_i <= cols_i).astype(F32)
    starts = jnp.broadcast_to(ds_ref[...].astype(F32), (8, tok))
    both = jnp.concatenate([lg_ref[...], starts], axis=0)
    cum_all = lax.dot_general(
        both, tri, NN, precision=lax.Precision.HIGHEST, preferred_element_type=F32
    )
    cum_t = jnp.transpose(cum_all)
    cum = cum_all[:heads]
    reset = cum_all[heads : heads + 1]
    reset_col = cum_t[:, heads : heads + 1]
    bias_s[...] = jnp.where((rows_i <= cols_i) & (reset == reset_col), 0.0, -1e30)
    end = cum[:, tok - 1 : tok]
    reset_end = reset[:, tok - 1 : tok]
    cum_s[...] = cum
    lead_s[...] = jnp.where(reset == 0, jnp.exp(cum), 0.0)
    tail_s[...] = jnp.where(reset == reset_end, jnp.exp(end - cum), 0.0)
    dec[0] = jnp.broadcast_to(jnp.where(reset_end == 0, jnp.exp(end), 0.0), (heads, dk))
    for h in range(heads):
        col_s[h] = jnp.broadcast_to(cum_t[:, h : h + 1], (tok, tok))

    def states(p, _):
        lanes = pl.ds(pl.multiple_of(p * dk, dk), dk)
        vt = jnp.transpose(v_ref[:, lanes].astype(F32))
        gt = jnp.transpose(g_ref[:, lanes].astype(F32))
        vt_s[p] = vt.astype(BF16)
        gt_s[p] = gt.astype(BF16)
        for i in range(group):
            h = p * group + i
            wide = pl.ds(pl.multiple_of(h * dk, dk), dk)
            part = slice(i * dv, (i + 1) * dv)
            tail = tail_s[pl.ds(h, 1), :]
            lead = lead_s[pl.ds(h, 1), :]
            state_s[h] = dot_fine(vt[part] * tail, k_ref[:, wide], NN)
            gw = jnp.concatenate(
                [gt[part] * (lead * lw_ref[l, pl.ds(h, 1), :]) for l in slots], axis=0
            )
            back = dot_fine(gw, q_ref[:, wide], NN)
            for n in range(len(slots)):
                back_s[n, h] = back[n * dv : (n + 1) * dv]
        return 0

    lax.fori_loop(0, pairs, states, 0, unroll=2)
    pl.semaphore_wait(barrier, seq_count - 1 + head_count - 1)

    def slot(b):
        return slots.index(cross[b])

    def remote(src, dst, send, recv, b):
        return pltpu.make_async_remote_copy(
            src_ref=src,
            dst_ref=dst,
            send_sem=send,
            recv_sem=recv,
            device_id={"seq": peer[b]},
            device_id_type=MESH,
        )

    own = pl.ds(mine, half)
    other = pl.ds(theirs, half)

    def u_copy(b, j):
        src = back_s.at[slot(j), other] if b == 0 else sum_u.at[b, j]
        return remote(src, got_u.at[b, j], u_send.at[b, j], u_recv.at[b, j], b)

    def s_copy(b):
        src = state_s.at[other] if b == 0 else sum_s.at[b]
        return remote(src, got_s.at[b], s_send.at[b], s_recv.at[b], b)

    def d_copy(b):
        return remote(dec.at[b], got_dec.at[b], d_send.at[b], d_recv.at[b], b)

    def level_copy(b, low):
        if b == 0:
            src = state_s if low else back_s.at[slot(0)]
            return [
                remote(src.at[part], lvl.at[0, part], lvl_send.at[0, n], lvl_recv.at[0, n], 0)
                for n, part in enumerate((other, own))
            ]
        src = sum_s.at[b] if low else sum_u.at[b, b]
        return [remote(src, lvl.at[b, own], lvl_send.at[b, 0], lvl_recv.at[b, 0], b)]

    def level_wait(b, n):
        part = other if n == 1 else own
        return remote(
            lvl.at[b, part], lvl.at[b, part], lvl_send.at[b, n], lvl_recv.at[b, n], b
        )

    def forward_copy(b, part):
        return remote(lvl.at[b, part], lvl.at[b, part], fwd_send.at[b], fwd_recv.at[b], 0)

    def land(b):
        up_summed = (bit[b] == 1) & want_s[b]

        @pl.when(jnp.logical_not(up_summed))
        def _():
            level_wait(b, 0).wait_recv()

        if b > 0:
            forward_copy(b, own).start()

    def begin(b):
        d_copy(b).start()

        early = 0 if b in (0, bits - 1) else 1

        @pl.when((bit[b] == 0) & (want_s[b] | (early == 0)))
        def _():
            for c in level_copy(b, True):
                c.start()

        if b < bits - 1:

            @pl.when((bit[b] == 1) & want_s[b])
            def _():
                s_copy(b).start()

            for j in range(b + 1, bits):

                @pl.when(bit[j] == 1)
                def _(j=j):
                    u_copy(b, j).start()

        if early == 0:

            @pl.when(bit[b] == 1)
            def _():
                for c in level_copy(b, False):
                    c.start()

    def begin_late(b):
        if b in (0, bits - 1):
            return

        @pl.when((bit[b] == 0) & jnp.logical_not(want_s[b]))
        def _():
            for c in level_copy(b, True):
                c.start()

        @pl.when(bit[b] == 1)
        def _():
            for c in level_copy(b, False):
                c.start()

    def join(b):
        d_copy(b).wait_recv()
        up = bit[b].astype(F32)
        got = got_dec[b]
        now = dec[b]
        dec[b + 1] = got * now
        if b == bits - 1:
            return
        base_s = state_s.at[own] if b == 0 else sum_s.at[b]

        @pl.when(want_s[b])
        def _():
            @pl.when(bit[b] == 1)
            def _():
                level_wait(b, 0).wait_recv()

                def body(i, _):
                    d = dec[b, pl.ds(mine + i, 1), :]
                    sum_s[b + 1, i] = d * lvl[b, mine + i] + base_s[i]
                    return 0

                lax.fori_loop(0, half, body, 0, unroll=True)

            @pl.when(bit[b] == 0)
            def _():
                s_copy(b).wait_recv()

                def body(i, _):
                    d = got_dec[b, pl.ds(mine + i, 1), :]
                    sum_s[b + 1, i] = d * base_s[i] + got_s[b, i]
                    return 0

                lax.fori_loop(0, half, body, 0, unroll=True)

        for j in range(b + 1, bits):
            base_u = back_s.at[slot(j), own] if b == 0 else sum_u.at[b, j]

            @pl.when(bit[j] == 1)
            def _(j=j, base_u=base_u):
                u_copy(b, j).wait_recv()

                def body(i, _):
                    d0 = dec[b, pl.ds(mine + i, 1), :]
                    d1 = got_dec[b, pl.ds(mine + i, 1), :]
                    a = up * d1 + (1.0 - up)
                    c = (1.0 - up) * d0 + up
                    sum_u[b + 1, j, i] = a * base_u[i] + c * got_u[b, j, i]
                    return 0

                lax.fori_loop(0, half, body, 0, unroll=True)

    span_of = lax.broadcasted_iota(jnp.int32, (1, tok), 1) // SPAN

    def local(p, _):
        vt = vt_s[p]
        gt = gt_s[p]
        lanes = pl.ds(pl.multiple_of(p * dk, dk), dk)
        v_blk = v_ref[:, lanes]
        for i in range(group):
            h = p * group + i
            wide = pl.ds(pl.multiple_of(h * dk, dk), dk)
            part = slice(i * dv, (i + 1) * dv)
            q = q_ref[:, wide]
            k = k_ref[:, wide]
            score = dot(k, q, NT)
            pair = dot(v_blk[:, part], gt[part], NN)
            decay = jnp.exp((cum_s[pl.ds(h, 1), :] - col_s[h]) + bias_s[...])
            seen = decay * score
            both_p = seen * pair
            gains = [lw_ref[l, pl.ds(h, 1), :] for l in range(span_bits + 1)]
            level_rows = [jnp.zeros((1, tok), F32) for _ in range(span_bits + 1)]
            mixed, graded = [], []
            for cs in range(spans):
                rows = slice(cs * SPAN, (cs + 1) * SPAN)
                total = jnp.sum(both_p[rows], axis=0, keepdims=True)
                gain = jnp.zeros((1, tok), F32)
                for ct in range(cs, spans):
                    l = span_level(cs, ct, levels)
                    hit = span_of == ct
                    gain = jnp.where(hit, gains[l], gain)
                    level_rows[l] = level_rows[l] + jnp.where(hit, total, 0.0)
                mixed.append(seen[rows] * gain)
                graded.append(decay[rows] * gain * pair[rows])
            mix = jnp.concatenate(mixed, axis=0).astype(BF16)
            grade = jnp.concatenate(graded, axis=0).astype(BF16)
            for l in range(span_bits + 1):
                gl_ref[l, pl.ds(h, 1), :] = level_rows[l]
            drift_s[pl.ds(h, 1), :] = jnp.sum(mix.astype(F32) * pair, axis=0, keepdims=True)
            vg_s[p, part] = dot(gt[part], mix, NT)
            gk_s[h] = dot(grade, q, NN)
            gq_s[h] = dot(grade, k, TN)
        return 0

    begin(0)
    lax.fori_loop(0, pairs // 4, local, 0, unroll=2)
    join(0)
    if bits > 1:
        begin(1)
    lax.fori_loop(pairs // 4, pairs, local, 0, unroll=2)
    for b in range(1, bits):
        join(b)
        if b + 1 < bits:
            begin(b + 1)
        begin_late(b)
        land(b - 1)
    land(bits - 1)

    inner_f = jnp.ones((heads, dk), F32)
    inner_b = jnp.ones((heads, dk), F32)
    for b in range(bits):
        up = bit[b].astype(F32)
        got = got_dec[b]
        coef_s[0, b] = inner_f * up
        coef_s[1, b] = inner_b * (1.0 - up)
        inner_f = inner_f * (up * got + (1.0 - up))
        inner_b = inner_b * ((1.0 - up) * got + up)
    level_wait(0, 1).wait_recv()
    for b in range(1, bits):
        forward_copy(b, other).wait_recv()

    def finish(p, _):
        lanes = pl.ds(pl.multiple_of(p * dk, dk), dk)
        vt = vt_s[p].astype(F32)
        gt = gt_s[p].astype(F32)
        vg_all = []
        for i in range(group):
            h = p * group + i
            wide = pl.ds(pl.multiple_of(h * dk, dk), dk)
            part = slice(i * dv, (i + 1) * dv)
            q = q_ref[:, wide]
            k = k_ref[:, wide]
            tail = tail_s[pl.ds(h, 1), :]
            lead = lead_s[pl.ds(h, 1), :]
            blocks = [lvl[b, h] for b in range(bits)]
            entering = []
            for n in range(len(slots)):
                terms = [
                    coef_s[0, b, pl.ds(h, 1), :] * blocks[b] for b in range(bits) if slot(b) == n
                ]
                entering.append(functools.reduce(jnp.add, terms))
            entering = jnp.concatenate(entering, axis=0)
            after = functools.reduce(
                jnp.add, [coef_s[1, b, pl.ds(h, 1), :] * blocks[b] for b in range(bits)]
            )
            e_high, e_low = split(entering)
            seen = dot(e_high, q, NT) + dot(e_low, q, NT)
            drift = drift_s[pl.ds(h, 1), :]
            gws = []
            for n, l in enumerate(slots):
                gain = lw_ref[l, pl.ds(h, 1), :]
                level = lead * jnp.sum(
                    seen[n * dv : (n + 1) * dv] * gt[part], axis=0, keepdims=True
                )
                gl_ref[l, pl.ds(h, 1), :] = level
                drift = drift + gain * level
                gws.append(gt[part] * (lead * gain))
            gw, gw_low = split(jnp.concatenate(gws, axis=0))
            gq_in = dot(gw, e_high, TN) + dot(gw, e_low, TN) + dot(gw_low, e_high, TN)
            gq_ref[:, wide] = (gq_s[h] + gq_in).astype(BF16)
            a_high, a_low = split(after)
            tv, tv_low = split(vt[part] * tail)
            gk_in = dot(tv, a_high, TN) + dot(tv, a_low, TN) + dot(tv_low, a_high, TN)
            gk_ref[:, wide] = (gk_s[h] + gk_in).astype(BF16)
            vg = vg_s[p, part] + tail * (dot(a_high, k, NT) + dot(a_low, k, NT))
            drift_s[pl.ds(h, 1), :] = drift - jnp.sum(vg * vt[part], axis=0, keepdims=True)
            vg_all.append(vg)
        gv_ref[:, lanes] = jnp.transpose(jnp.concatenate(vg_all, axis=0)).astype(BF16)
        return 0

    lax.fori_loop(0, pairs, finish, 0, unroll=2)
    for l in range(levels):
        if l > span_bits and l not in slots:
            gl_ref[l] = jnp.zeros((heads, tok), F32)

    later = (rows_i >= cols_i).astype(F32)
    local_tail = lax.dot_general(
        drift_s[...], later, NN, precision=lax.Precision.HIGHEST, preferred_element_type=F32
    )
    lane = lax.broadcasted_iota(jnp.int32, (heads, tok), 1)
    first = local_tail[:, 0:1]
    plain = jnp.sum(local_tail, axis=1, keepdims=True)
    square = jnp.sum(local_tail * local_tail, axis=1, keepdims=True)
    tot[place] = jnp.where(lane == 0, first, jnp.where(lane == 1, plain, square))

    def tot_copy(o, slot_at):
        return pltpu.make_async_remote_copy(
            src_ref=tot.at[place],
            dst_ref=tot.at[slot_at],
            send_sem=t_send.at[o],
            recv_sem=t_recv.at[slot_at],
            device_id={"seq": (place + o) % seq_count},
            device_id_type=MESH,
        )

    for o in range(1, seq_count):
        tot_copy(o, place).start()
    for o in range(1, seq_count):
        tot_copy(o, (place + o) % seq_count).wait_recv()
    after_total = jnp.zeros((heads, 1), F32)
    my_later = jnp.zeros((heads, 1), F32)
    energy = jnp.zeros((heads, 1), F32)
    for d in reversed(range(seq_count)):
        piece = tot[d]
        my_later = my_later + jnp.where(place == d, 1.0, 0.0) * after_total
        energy = energy + (
            piece[:, 2:3] + after_total * (2.0 * piece[:, 1:2] + tok * after_total)
        )
        after_total = after_total + piece[:, 0:1]
    energy = jnp.sum(jnp.broadcast_to(energy, (heads, dk)), axis=0, keepdims=True)
    sq[row] = jnp.broadcast_to(energy, (8, dk))

    def sq_copy(o, slot_at):
        return pltpu.make_async_remote_copy(
            src_ref=sq.at[row],
            dst_ref=sq.at[slot_at],
            send_sem=q_send.at[o],
            recv_sem=q_recv.at[slot_at],
            device_id={"head": (row + o) % head_count},
            device_id_type=MESH,
        )

    for o in range(1, head_count):
        sq_copy(o, row).start()
    for o in range(1, head_count):
        sq_copy(o, (row + o) % head_count).wait_recv()
    whole = sq[0]
    for r in range(1, head_count):
        whole = whole + sq[r]
    count = heads * tok * seq_count * head_count
    factor = jnp.minimum(1.0, lax.rsqrt(whole[0:1] / count + 1e-6))
    gg_ref[...] = (local_tail + my_later) * factor

    for b in range(bits):
        d_copy(b).wait_send()
        for n in range(2 if b == 0 else 1):
            level_wait(b, n).wait_send()
        if b > 0:
            forward_copy(b, own).wait_send()
        if b < bits - 1:

            @pl.when((bit[b] == 1) & want_s[b])
            def _(b=b):
                s_copy(b).wait_send()

            for j in range(b + 1, bits):

                @pl.when(bit[j] == 1)
                def _(b=b, j=j):
                    u_copy(b, j).wait_send()

    for o in range(1, seq_count):
        tot_copy(o, place).wait_send()
    for o in range(1, head_count):
        sq_copy(o, row).wait_send()


def shards(seq_count, head_count, queries, keys, values, out_grad, log_gate, level_weight, doc_start):
    tok = queries.shape[0]
    heads = log_gate.shape[0]
    levels = level_weight.shape[0]
    dk = queries.shape[1] // heads
    dv = values.shape[1] // heads
    group = dk // dv
    pairs = heads // group
    bits = seq_count.bit_length() - 1
    half = heads // 2
    span_bits = (tok // SPAN).bit_length() - 1
    slots = len({min(span_bits + 1 + b, levels - 1) for b in range(bits)})
    dma = pltpu.SemaphoreType.DMA
    vmem = pltpu.VMEM
    block = (dv, dk)
    scratch = [
        vmem((heads, tok), F32),
        vmem((heads, tok, tok), F32),
        vmem((heads, tok), F32),
        vmem((heads, tok), F32),
        vmem((tok, tok), F32),
        vmem((pairs, group * dv, tok), BF16),
        vmem((pairs, group * dv, tok), BF16),
        vmem((pairs, group * dv, tok), F32),
        vmem((heads, tok, dk), F32),
        vmem((heads, tok, dk), F32),
        vmem((heads, tok), F32),
        vmem((2, bits, heads, dk), F32),
        vmem((heads,) + block, F32),
        vmem((slots, heads) + block, F32),
        vmem((bits, heads) + block, F32),
        vmem((bits, half) + block, F32),
        vmem((bits, bits, half) + block, F32),
        vmem((bits, half) + block, F32),
        vmem((bits, bits, half) + block, F32),
        vmem((bits + 1, heads, dk), F32),
        vmem((bits, heads, dk), F32),
        vmem((seq_count, heads, tok), F32),
        vmem((head_count, 8, dk), F32),
        dma((bits, 2)),
        dma((bits, 2)),
        dma((bits,)),
        dma((bits,)),
        dma((bits,)),
        dma((bits,)),
        dma((bits, bits)),
        dma((bits, bits)),
        dma((bits,)),
        dma((bits,)),
        dma((seq_count,)),
        dma((seq_count,)),
        dma((head_count,)),
        dma((head_count,)),
    ]
    spec = pl.BlockSpec(memory_space=pltpu.VMEM)
    return pl.pallas_call(
        functools.partial(kernel, seq_count, head_count),
        out_shape=(
            jax.ShapeDtypeStruct(queries.shape, BF16),
            jax.ShapeDtypeStruct(keys.shape, BF16),
            jax.ShapeDtypeStruct(values.shape, BF16),
            jax.ShapeDtypeStruct(level_weight.shape, F32),
            jax.ShapeDtypeStruct(log_gate.shape, F32),
        ),
        in_specs=[spec] * 7,
        out_specs=(spec,) * 5,
        scratch_shapes=scratch,
        compiler_params=pltpu.CompilerParams(collective_id=0, has_side_effects=True),
    )(queries, keys, values, out_grad, log_gate, level_weight, doc_start.reshape(1, tok))


def solution(mesh):
    return jax.shard_map(
        functools.partial(shards, mesh.shape["seq"], mesh.shape["head"]),
        mesh=mesh,
        in_specs=(
            P("seq", "head"),
            P("seq", "head"),
            P("seq", "head"),
            P("seq", "head"),
            P("head", "seq"),
            P(None, "head", "seq"),
            P("seq"),
        ),
        out_specs=(
            P("seq", "head"),
            P("seq", "head"),
            P("seq", "head"),
            P(None, "head", "seq"),
            P("head", "seq"),
        ),
        check_vma=False,
    )
```
